32 devices in a mesh: cls: 8 (over z, y), row: 4 (over x, core).
Axes of the slice: x: 2, y: 2, z: 4, core: 2. Of those that a mesh axis runs over, the one named last changes fastest.
Arguments:
- embeddings: float32 [1024, 1024], P('row'), may hold values from -6 to 6
- weights: float32 [1024, 81920], P(('cls', 'row')), may hold values from -4 to 4
- labels: int32 [1024], replicated, may hold values from 0 to 81919, as said below
Outputs:
- weight_update: float32 [1024, 81920], P(None, ('cls', 'row'))
- losses: float32 [2, 1024], replicated
The draws below stay inside these ranges and needn't reach their ends.
Inputs may be any that keep to these rules, and one draw needn't show every extreme that they name: labels take at most 512 distinct values, at most one in each aligned run of 160 classes; rows may share a label.
All inputs are finite; a program needn't handle non-finite values.
Results may differ from the reference program's by a relative error of at most 0.012.
The reference program's roundings to bfloat16 on the way count: a program that leaves them out, or rounds other values in their place, can miss the bound.
Values may be sent and summed in bfloat16 or wider, within the bound.
A program may use at most 128 MiB of HBM per device.

```python
import math
import jax
import jax.numpy as jnp
from jax import lax

D = 1024
CLS_DEV = 2560
STEPS = 2
ROWS = 1024
CLASSES = 81920


def embedding_draw(key):
    noise = jax.random.normal(jax.random.fold_in(key, 7), (ROWS, D), jnp.float32)
    return jnp.clip(noise + 0.5, -6.0, 6.0)


def draw_embeddings(key, part):
    return embedding_draw(key)


def draw_weights(key, part):
    base = jax.random.normal(jax.random.fold_in(key, 9), (D, CLASSES), jnp.float32) * (8.0 / math.sqrt(D))
    base = jnp.clip(base, -4.0, 4.0)
    return base


def draw_labels(key, part):
    run_width = CLASSES // 512
    slots = jax.random.randint(jax.random.fold_in(key, 21), (ROWS,), 0, 512, dtype=jnp.int32)
    slots = slots.at[0].set(0).at[ROWS - 1].set(511)
    offsets = jax.random.randint(jax.random.fold_in(key, 22), (512,), 0, run_width, dtype=jnp.int32)
    offsets = offsets.at[0].set(0).at[511].set(run_width - 1)
    return (slots * run_width + offsets[slots]).astype(jnp.int32)


def setup_inputs(seed: int = 0) -> dict:
    arg_keys = jax.random.split(jax.random.key(seed), 4)
    return {
        "embeddings": draw_embeddings(jax.random.fold_in(arg_keys[3], 71), 0),
        "weights": draw_weights(jax.random.fold_in(arg_keys[3], 71), 0),
        "labels": draw_labels(jax.random.fold_in(arg_keys[3], 71), 0),
    }


learn_rate = 2.0


def reference(embeddings, weights, labels):
    rounded = embeddings.astype(jnp.bfloat16)
    row_count = rounded.shape[0]
    block_count = CLASSES // CLS_DEV
    columns = jnp.arange(CLS_DEV, dtype=jnp.int32)
    starts = jnp.arange(block_count, dtype=jnp.int32) * CLS_DEV
    current = weights
    loss_rows = []
    for step_index in range(STEPS):
        stacked = current.reshape(D, block_count, CLS_DEV).transpose(1, 0, 2)

        def block_stats(operands):
            class_block, start = operands
            logits = jnp.dot(rounded, class_block.astype(jnp.bfloat16), preferred_element_type=jnp.float32)
            block_peak = jnp.max(logits, axis=1)
            block_total = jnp.sum(jnp.exp(logits - block_peak[:, None]), axis=1)
            label_hit = (columns[None, :] + start) == labels[:, None]
            block_picked = jnp.sum(jnp.where(label_hit, logits, jnp.float32(0.0)), axis=1)
            return block_peak, block_total, block_picked

        peaks, totals, pickeds = lax.map(block_stats, (stacked, starts))
        row_peak = jnp.max(peaks, axis=0)
        row_total = jnp.sum(totals * jnp.exp(peaks - row_peak[None, :]), axis=0)
        picked = jnp.sum(pickeds, axis=0)
        log_norm = row_peak + jnp.log(row_total)
        loss_rows.append(log_norm - picked)

        def block_update(operands):
            class_block, start = operands
            logits = jnp.dot(rounded, class_block.astype(jnp.bfloat16), preferred_element_type=jnp.float32)
            label_hit = (columns[None, :] + start) == labels[:, None]
            onehot = jnp.where(label_hit, jnp.float32(1.0), jnp.float32(0.0))
            residual = (jnp.exp(logits - log_norm[:, None]) - onehot).astype(jnp.bfloat16)
            gradient = jnp.dot(rounded.T, residual, preferred_element_type=jnp.float32) / row_count
            return class_block - learn_rate * gradient

        renewed = lax.map(block_update, (stacked, starts))
        current = renewed.transpose(1, 0, 2).reshape(D, CLASSES)
    return current - weights, jnp.stack(loss_rows)
```

```python
import jax
import jax.numpy as jnp
from jax import lax
from jax.sharding import PartitionSpec as P

STEPS = 2


learn_rate = 2.0


def shards(embeddings, weights, labels):
    peer_count = lax.axis_size(("cls", "row"))
    examples = lax.all_gather(embeddings.astype(jnp.bfloat16), "row", axis=0, tiled=True)
    row_count = examples.shape[0]
    feature_rows = weights.shape[0]
    class_count = weights.shape[1] // peer_count
    offset = lax.axis_index(("cls", "row")) * class_count
    columns = lax.broadcasted_iota(jnp.int32, (1, class_count), 1) + offset
    label_hit = columns == labels[:, None]
    pieces = weights.astype(jnp.bfloat16).reshape(feature_rows, peer_count, class_count)
    block_weights = lax.all_to_all(
        pieces.transpose(1, 0, 2), ("cls", "row"), split_axis=0, concat_axis=0, tiled=True
    )
    flat_weights = block_weights.reshape(peer_count * feature_rows, class_count)
    first_logits = jnp.dot(examples, flat_weights, preferred_element_type=jnp.float32)
    rate = learn_rate / row_count
    gram = lax.dot_general(
        examples, examples, (((1,), (1,)), ((), ())), preferred_element_type=jnp.float32
    ).astype(jnp.bfloat16)
    total = None
    loss_rows = []
    for step_index in range(STEPS):
        logits = first_logits
        if step_index > 0:
            logits = logits - rate * jnp.dot(gram, total, preferred_element_type=jnp.float32)
        local_peak = jnp.max(logits, axis=1)
        local_total = jnp.sum(jnp.exp(logits - local_peak[:, None]), axis=1)
        local_picked = jnp.sum(jnp.where(label_hit, logits, 0.0), axis=1)
        stats = lax.all_gather(
            jnp.stack([local_peak, local_total, local_picked]), ("cls", "row"), axis=0
        )
        row_peak = jnp.max(stats[:, 0], axis=0)
        row_total = jnp.sum(stats[:, 1] * jnp.exp(stats[:, 0] - row_peak[None, :]), axis=0)
        picked = jnp.sum(stats[:, 2], axis=0)
        log_norm = row_peak + jnp.log(row_total)
        loss_rows.append(log_norm - picked)
        onehot = jnp.where(label_hit, 1.0, 0.0)
        residual = jnp.exp(logits - log_norm[:, None]) - onehot
        if total is not None:
            residual = residual + total.astype(jnp.float32)
        total = residual.astype(jnp.bfloat16)
    update = lax.dot_general(
        examples, total, (((0,), (0,)), ((), ())), preferred_element_type=jnp.float32
    )
    return (-rate * update, jnp.stack(loss_rows))


def solution(mesh):
    placed = (P("row", None), P(("cls", "row"), None), P())
    return jax.shard_map(
        shards,
        mesh=mesh,
        in_specs=placed,
        out_specs=(P(None, ("cls", "row")), P()),
        check_vma=False,
    )
```

```python
import functools

import jax
import jax.numpy as jnp
from jax import lax
from jax.experimental import pallas as pl
from jax.experimental.pallas import tpu as pltpu
from jax.sharding import PartitionSpec as P

STEPS = 2


learn_rate = 2.0

MESH = pl.DeviceIdType.MESH
LANES = 128
ROW_TILE = 256
SUB = 32


def exchange_kernel(
    cls_n,
    row_n,
    rate,
    emb_ref,
    weights_ref,
    labels_ref,
    total_ref,
    turned_ref,
    losses_ref,
    stage,
    outgoing,
    incoming,
    logits,
    gram,
    examples,
    emb_bf,
    peak_lanes,
    sum_lanes,
    pick_lanes,
    norm_lanes,
    row_send,
    row_recv,
    cls_send,
    cls_recv,
    load_sem,
    out_sem,
    in_sem,
    emb_out,
    emb_in,
    row_out,
    row_in,
    cls_out,
    cls_in,
):
    n = cls_n * row_n
    my_cls, my_row = lax.axis_index("cls"), lax.axis_index("row")
    me = my_cls * row_n + my_row
    chunks, rows, width = logits.shape
    features = outgoing.shape[2]
    class_count = chunks * width
    shard_rows = emb_ref.shape[0]
    tiles = rows // ROW_TILE
    groups = width // LANES
    slabs = rows // LANES

    def place(p):
        return (lax.div(p, row_n), lax.rem(p, row_n))

    def load(chunk, slot):
        @pl.loop(0, n)
        def _(p):
            start = pl.multiple_of(p * class_count + chunk * width, LANES)
            pltpu.make_async_copy(
                weights_ref.at[:, pl.ds(start, width)], stage.at[slot, p], load_sem.at[slot]
            ).start()

    load(0, 0)
    load(1, 1)

    barrier = pltpu.get_barrier_semaphore()

    @pl.loop(1, n)
    def _(k):
        pl.semaphore_signal(
            barrier, inc=1, device_id=place(lax.rem(me + k, n)), device_id_type=MESH
        )

    emb_bf[...] = emb_ref[...].astype(jnp.bfloat16)
    mine = pl.ds(pl.multiple_of(my_row * shard_rows, shard_rows), shard_rows)
    examples[mine, :] = emb_bf[...]
    pl.semaphore_wait(barrier, n - 1)

    @pl.loop(0, chunks)
    def _(c):
        slot = lax.rem(c, 2)
        pltpu.make_async_copy(stage.at[slot], stage.at[slot], load_sem.at[slot]).wait()
        spot = pl.ds(pl.multiple_of(me * features, features), features)

        def send(j):
            p = lax.rem(me + j + n // 2, n)
            outgoing[c, p] = stage[slot, p].astype(jnp.bfloat16)
            pltpu.make_async_remote_copy(
                src_ref=outgoing.at[c, p],
                dst_ref=incoming.at[c, spot],
                send_sem=out_sem.at[c],
                recv_sem=in_sem.at[c],
                device_id=place(p),
                device_id_type=MESH,
            ).start()

        pl.loop(0, n // 2)(send)
        incoming[c, spot] = stage[slot, me].astype(jnp.bfloat16)
        pl.loop(n // 2 + 1, n)(send)

        @pl.when(c == 0)
        def _():
            @pl.loop(1, row_n)
            def _(k):
                pltpu.make_async_remote_copy(
                    src_ref=emb_bf,
                    dst_ref=examples.at[mine],
                    send_sem=emb_out,
                    recv_sem=emb_in,
                    device_id=(my_cls, lax.rem(my_row + k, row_n)),
                    device_id_type=MESH,
                ).start()

        @pl.when(c + 2 < chunks)
        def _():
            load(c + 2, slot)

    peers = pl.ds(0, (row_n - 1) * shard_rows)
    pltpu.make_async_copy(examples.at[peers], examples.at[peers], emb_in).wait()

    @pl.loop(0, tiles)
    def _(i):
        here = pl.ds(pl.multiple_of(i * ROW_TILE, ROW_TILE), ROW_TILE)
        gram[here, :] = lax.dot_general(
            examples[here, :],
            examples[...],
            (((1,), (1,)), ((), ())),
            preferred_element_type=jnp.float32,
        ).astype(jnp.bfloat16)
        turned_ref[:, here] = examples[here, :].astype(jnp.float32).T.astype(jnp.bfloat16)

    lane = lax.broadcasted_iota(jnp.int32, (SUB, LANES), 1)

    def reset():
        peak_lanes[...] = jnp.full_like(peak_lanes, -3.0e38)
        sum_lanes[...] = jnp.zeros_like(sum_lanes)
        pick_lanes[...] = jnp.zeros_like(pick_lanes)

    def hits(spot, c):
        shifted = labels_ref[spot, :] - c * width
        return [lane + q * LANES == shifted for q in range(groups)]

    def collect(c, i):
        @pl.loop(0, ROW_TILE // SUB, unroll=2)
        def _(u):
            spot = pl.ds(pl.multiple_of(i * ROW_TILE + u * SUB, SUB), SUB)
            block = logits[c, spot, :]
            parts = [block[:, q * LANES : (q + 1) * LANES] for q in range(groups)]
            old = peak_lanes[spot, :]
            peak = functools.reduce(jnp.maximum, parts, old)
            total = sum_lanes[spot, :] * jnp.exp(old - peak)
            picked = pick_lanes[spot, :]
            for part, hit in zip(parts, hits(spot, c)):
                total = total + jnp.exp(part - peak)
                picked = picked + jnp.where(hit, part, 0.0)
            peak_lanes[spot, :] = peak
            sum_lanes[spot, :] = total
            pick_lanes[spot, :] = picked

    def share(t, send_buf, recv_buf, send_sem, recv_sem, count, mine_at, target):
        recv_buf[t, mine_at] = send_buf[t]

        @pl.loop(1, count)
        def _(k):
            pltpu.make_async_remote_copy(
                src_ref=send_buf.at[t],
                dst_ref=recv_buf.at[t, mine_at],
                send_sem=send_sem.at[t],
                recv_sem=recv_sem.at[t],
                device_id=target(k),
                device_id_type=MESH,
            ).start()

        every = pl.ds(0, count - 1)
        pltpu.make_async_copy(recv_buf.at[t, every], recv_buf.at[t, every], recv_sem.at[t]).wait()
        norms = recv_buf[t, :, :slabs, :]
        top = jnp.max(norms, axis=0)
        norm = top + jnp.log(jnp.sum(jnp.exp(norms - top[None]), axis=0))
        picked = jnp.sum(recv_buf[t, :, slabs:, :], axis=0)
        pltpu.make_async_copy(recv_buf.at[t, every], recv_buf.at[t, every], send_sem.at[t]).wait()
        return norm, picked

    def settle(t):
        for i in range(slabs):
            part = pl.ds(i * LANES, LANES)
            peaks = peak_lanes[part, :].T
            top = jnp.max(peaks, axis=0, keepdims=True)
            total = jnp.sum(sum_lanes[part, :].T * jnp.exp(peaks - top), axis=0, keepdims=True)
            row_send[t, i : i + 1, :] = top + jnp.log(total)
            row_send[t, slabs + i : slabs + i + 1, :] = jnp.sum(
                pick_lanes[part, :].T, axis=0, keepdims=True
            )
        norm, picked = share(
            t, row_send, row_recv, row_out, row_in, row_n, my_row,
            lambda k: (my_cls, lax.rem(my_row + k, row_n)),
        )
        cls_send[t, :slabs, :] = norm
        cls_send[t, slabs:, :] = picked
        norm, picked = share(
            t, cls_send, cls_recv, cls_out, cls_in, cls_n, my_cls,
            lambda k: (lax.rem(my_cls + k, cls_n), my_row),
        )
        losses_ref[t] = norm - picked
        for i in range(slabs):
            norm_lanes[pl.ds(i * LANES, LANES), :] = jnp.broadcast_to(
                norm[i : i + 1, :], (LANES, LANES)
            ).T

    def residuals(first):
        @pl.loop(0, chunks)
        def _(c):
            @pl.loop(0, rows // SUB, unroll=2)
            def _(u):
                spot = pl.ds(pl.multiple_of(u * SUB, SUB), SUB)
                norm = norm_lanes[spot, :]
                block = logits[c, spot, :]
                for q, hit in enumerate(hits(spot, c)):
                    columns = slice(q * LANES, (q + 1) * LANES)
                    value = jnp.exp(block[:, columns] - norm) - jnp.where(hit, 1.0, 0.0)
                    if not first:
                        value = value + total_ref[c, spot, columns].astype(jnp.float32)
                    total_ref[c, spot, columns] = value.astype(jnp.bfloat16)

    reset()

    @pl.loop(0, chunks)
    def _(c):
        arrived = pl.ds(0, (n - 1) * features)
        pltpu.make_async_copy(
            incoming.at[c, arrived], incoming.at[c, arrived], in_sem.at[c]
        ).wait()

        @pl.loop(0, tiles)
        def _(i):
            here = pl.ds(pl.multiple_of(i * ROW_TILE, ROW_TILE), ROW_TILE)
            logits[c, here, :] = jnp.dot(
                examples[here, :], incoming[c], preferred_element_type=jnp.float32
            )
            collect(c, i)

    settle(0)
    residuals(True)
    for t in range(1, STEPS):
        reset()

        @pl.loop(0, chunks)
        def _(c):
            @pl.loop(0, tiles)
            def _(i):
                here = pl.ds(pl.multiple_of(i * ROW_TILE, ROW_TILE), ROW_TILE)
                change = jnp.dot(
                    gram[here, :], total_ref[c], preferred_element_type=jnp.float32
                )
                logits[c, here, :] = logits[c, here, :] - rate * change
                collect(c, i)

        settle(t)
        residuals(False)

    pltpu.make_async_copy(examples.at[peers], examples.at[peers], emb_out).wait()

    @pl.loop(0, chunks)
    def _(c):
        sent = pl.ds(0, n - 1)
        pltpu.make_async_copy(outgoing.at[c, sent], outgoing.at[c, sent], out_sem.at[c]).wait()


def update_kernel(rate, turned_ref, total_ref, out_ref):
    out_ref[...] = -rate * jnp.dot(
        turned_ref[...], total_ref[0], preferred_element_type=jnp.float32
    )


def fused(embeddings, weights, labels):
    cls_n, row_n = lax.axis_size("cls"), lax.axis_size("row")
    n = cls_n * row_n
    shard_rows, model_width = embeddings.shape
    rows = shard_rows * row_n
    features = weights.shape[0]
    class_count = weights.shape[1] // n
    width = max(w for w in (128, 256, 384, 512) if class_count % w == 0)
    chunks = class_count // width
    rate = learn_rate / rows
    slabs = rows // LANES
    offset = lax.axis_index(("cls", "row")) * class_count
    label_lanes = jnp.broadcast_to((labels - offset)[:, None], (rows, LANES))
    vmem = pl.BlockSpec(memory_space=pltpu.VMEM)
    dma = pltpu.SemaphoreType.DMA
    total, turned, losses = pl.pallas_call(
        functools.partial(exchange_kernel, cls_n, row_n, rate),
        out_shape=(
            jax.ShapeDtypeStruct((chunks, rows, width), jnp.bfloat16),
            jax.ShapeDtypeStruct((model_width, rows), jnp.bfloat16),
            jax.ShapeDtypeStruct((STEPS, slabs, LANES), jnp.float32),
        ),
        in_specs=[vmem, pl.BlockSpec(memory_space=pl.ANY), vmem],
        out_specs=(vmem, vmem, vmem),
        scratch_shapes=[
            pltpu.VMEM((2, n, features, width), jnp.float32),
            pltpu.VMEM((chunks, n, features, width), jnp.bfloat16),
            pltpu.VMEM((chunks, n * features, width), jnp.bfloat16),
            pltpu.VMEM((chunks, rows, width), jnp.float32),
            pltpu.VMEM((rows, rows), jnp.bfloat16),
            pltpu.VMEM((rows, model_width), jnp.bfloat16),
            pltpu.VMEM((shard_rows, model_width), jnp.bfloat16),
            pltpu.VMEM((rows, LANES), jnp.float32),
            pltpu.VMEM((rows, LANES), jnp.float32),
            pltpu.VMEM((rows, LANES), jnp.float32),
            pltpu.VMEM((rows, LANES), jnp.float32),
            pltpu.VMEM((STEPS, 2 * slabs, LANES), jnp.float32),
            pltpu.VMEM((STEPS, row_n, 2 * slabs, LANES), jnp.float32),
            pltpu.VMEM((STEPS, 2 * slabs, LANES), jnp.float32),
            pltpu.VMEM((STEPS, cls_n, 2 * slabs, LANES), jnp.float32),
            dma((2,)),
            dma((chunks,)),
            dma((chunks,)),
            dma,
            dma,
            dma((STEPS,)),
            dma((STEPS,)),
            dma((STEPS,)),
            dma((STEPS,)),
        ],
        compiler_params=pltpu.CompilerParams(
            collective_id=0, has_side_effects=True, vmem_limit_bytes=60 * 1024 * 1024
        ),
    )(embeddings, weights, label_lanes)
    tall = model_width // 2
    update = pl.pallas_call(
        functools.partial(update_kernel, rate),
        grid=(chunks, 2),
        out_shape=jax.ShapeDtypeStruct((model_width, class_count), jnp.float32),
        in_specs=[
            pl.BlockSpec((tall, rows), lambda c, i: (i, 0)),
            pl.BlockSpec((1, rows, width), lambda c, i: (c, 0, 0)),
        ],
        out_specs=pl.BlockSpec((tall, width), lambda c, i: (i, c)),
        compiler_params=pltpu.CompilerParams(
            dimension_semantics=("arbitrary", "arbitrary"), vmem_limit_bytes=32 * 1024 * 1024
        ),
    )(turned, total)
    return update, losses.reshape(STEPS, rows)


def shards(embeddings, weights, labels):
    if STEPS == 2 and weights.shape[0] % 16 == 0:
        return fused(embeddings, weights, labels)
    peer_count = lax.axis_size(("cls", "row"))
    examples = lax.all_gather(embeddings.astype(jnp.bfloat16), "row", axis=0, tiled=True)
    row_count = examples.shape[0]
    feature_rows = weights.shape[0]
    class_count = weights.shape[1] // peer_count
    offset = lax.axis_index(("cls", "row")) * class_count
    columns = lax.broadcasted_iota(jnp.int32, (1, class_count), 1) + offset
    label_hit = columns == labels[:, None]
    pieces = weights.astype(jnp.bfloat16).reshape(feature_rows, peer_count, class_count)
    block_weights = lax.all_to_all(
        pieces.transpose(1, 0, 2), ("cls", "row"), split_axis=0, concat_axis=0, tiled=True
    )
    flat_weights = block_weights.reshape(peer_count * feature_rows, class_count)
    first_logits = jnp.dot(examples, flat_weights, preferred_element_type=jnp.float32)
    rate = learn_rate / row_count
    gram = lax.dot_general(
        examples, examples, (((1,), (1,)), ((), ())), preferred_element_type=jnp.float32
    ).astype(jnp.bfloat16)
    total = None
    loss_rows = []
    for step_index in range(STEPS):
        logits = first_logits
        if step_index > 0:
            logits = logits - rate * jnp.dot(gram, total, preferred_element_type=jnp.float32)
        local_peak = jnp.max(logits, axis=1)
        local_total = jnp.sum(jnp.exp(logits - local_peak[:, None]), axis=1)
        local_picked = jnp.sum(jnp.where(label_hit, logits, 0.0), axis=1)
        stats = lax.all_gather(
            jnp.stack([local_peak, local_total, local_picked]), ("cls", "row"), axis=0
        )
        row_peak = jnp.max(stats[:, 0], axis=0)
        row_total = jnp.sum(stats[:, 1] * jnp.exp(stats[:, 0] - row_peak[None, :]), axis=0)
        picked = jnp.sum(stats[:, 2], axis=0)
        log_norm = row_peak + jnp.log(row_total)
        loss_rows.append(log_norm - picked)
        onehot = jnp.where(label_hit, 1.0, 0.0)
        residual = jnp.exp(logits - log_norm[:, None]) - onehot
        if total is not None:
            residual = residual + total.astype(jnp.float32)
        total = residual.astype(jnp.bfloat16)
    update = lax.dot_general(
        examples, total, (((0,), (0,)), ((), ())), preferred_element_type=jnp.float32
    )
    return (-rate * update, jnp.stack(loss_rows))


def solution(mesh):
    placed = (P("row", None), P(("cls", "row"), None), P())
    return jax.shard_map(
        shards,
        mesh=mesh,
        in_specs=placed,
        out_specs=(P(None, ("cls", "row")), P()),
        check_vma=False,
    )
```

```python
import functools

import jax
import jax.numpy as jnp
from jax import lax
from jax.experimental import pallas as pl
from jax.experimental.pallas import tpu as pltpu
from jax.sharding import PartitionSpec as P

STEPS = 2


learn_rate = 2.0

MESH = pl.DeviceIdType.MESH
LANES = 128
ROW_TILE = 256
SUB = 32


def exchange_kernel(
    cls_n,
    row_n,
    rate,
    emb_ref,
    weights_ref,
    labels_ref,
    total_ref,
    turned_ref,
    losses_ref,
    stage,
    outgoing,
    incoming,
    label_lanes,
    logits,
    gram,
    examples,
    emb_bf,
    peak_lanes,
    sum_lanes,
    pick_lanes,
    norm_lanes,
    row_send,
    row_recv,
    cls_send,
    cls_recv,
    load_sem,
    out_sem,
    in_sem,
    emb_out,
    emb_in,
    row_out,
    row_in,
    cls_out,
    cls_in,
):
    n = cls_n * row_n
    my_cls, my_row = lax.axis_index("cls"), lax.axis_index("row")
    me = my_cls * row_n + my_row
    chunks, rows, width = logits.shape
    features = outgoing.shape[2]
    class_count = chunks * width
    shard_rows = emb_ref.shape[0]
    tiles = rows // ROW_TILE
    groups = width // LANES
    slabs = rows // LANES

    def place(p):
        return (lax.div(p, row_n), lax.rem(p, row_n))

    def load(chunk, slot):
        @pl.loop(0, n)
        def _(p):
            start = pl.multiple_of(p * class_count + chunk * width, LANES)
            pltpu.make_async_copy(
                weights_ref.at[:, pl.ds(start, width)], stage.at[slot, p], load_sem.at[slot]
            ).start()

    load(0, 0)
    load(1, 1)

    barrier = pltpu.get_barrier_semaphore()

    @pl.loop(1, n)
    def _(k):
        pl.semaphore_signal(
            barrier, inc=1, device_id=place(lax.rem(me + k, n)), device_id_type=MESH
        )

    emb_bf[...] = emb_ref[...].astype(jnp.bfloat16)
    mine = pl.ds(pl.multiple_of(my_row * shard_rows, shard_rows), shard_rows)
    examples[mine, :] = emb_bf[...]
    pl.semaphore_wait(barrier, n - 1)

    @pl.loop(0, chunks)
    def _(c):
        slot = lax.rem(c, 2)
        pltpu.make_async_copy(stage.at[slot], stage.at[slot], load_sem.at[slot]).wait()
        spot = pl.ds(pl.multiple_of(me * features, features), features)

        def send(j):
            p = lax.rem(me + j + n // 2, n)
            outgoing[c, p] = stage[slot, p].astype(jnp.bfloat16)
            pltpu.make_async_remote_copy(
                src_ref=outgoing.at[c, p],
                dst_ref=incoming.at[c, spot],
                send_sem=out_sem.at[c],
                recv_sem=in_sem.at[c],
                device_id=place(p),
                device_id_type=MESH,
            ).start()

        pl.loop(0, n // 2)(send)
        incoming[c, spot] = stage[slot, me].astype(jnp.bfloat16)
        pl.loop(n // 2 + 1, n)(send)

        @pl.when(c == 0)
        def _():
            @pl.loop(1, row_n)
            def _(k):
                pltpu.make_async_remote_copy(
                    src_ref=emb_bf,
                    dst_ref=examples.at[mine],
                    send_sem=emb_out,
                    recv_sem=emb_in,
                    device_id=(my_cls, lax.rem(my_row + k, row_n)),
                    device_id_type=MESH,
                ).start()

        @pl.when(c + 2 < chunks)
        def _():
            load(c + 2, slot)

    peers = pl.ds(0, (row_n - 1) * shard_rows)
    pltpu.make_async_copy(examples.at[peers], examples.at[peers], emb_in).wait()

    @pl.loop(0, tiles)
    def _(i):
        here = pl.ds(pl.multiple_of(i * ROW_TILE, ROW_TILE), ROW_TILE)
        gram[here, :] = lax.dot_general(
            examples[here, :],
            examples[...],
            (((1,), (1,)), ((), ())),
            preferred_element_type=jnp.float32,
        ).astype(jnp.bfloat16)
        turned_ref[:, here] = examples[here, :].astype(jnp.float32).T.astype(jnp.bfloat16)

    for i in range(slabs):
        label_lanes[pl.ds(i * LANES, LANES), :] = (
            jnp.broadcast_to(labels_ref[i : i + 1, :], (LANES, LANES)).T - me * class_count
        )

    def reset():
        peak_lanes[...] = jnp.full_like(peak_lanes, -3.0e38)
        sum_lanes[...] = jnp.zeros_like(sum_lanes)
        pick_lanes[...] = jnp.zeros_like(pick_lanes)

    def hits(spot, c):
        shifted = label_lanes[spot, :] - c * width
        lane = lax.broadcasted_iota(jnp.int32, shifted.shape, 1)
        return [lane + q * LANES == shifted for q in range(groups)]

    def collect(c, spot, block):
        parts = [block[:, q * LANES : (q + 1) * LANES] for q in range(groups)]
        old = peak_lanes[spot, :]
        peak = functools.reduce(jnp.maximum, parts, old)
        total = sum_lanes[spot, :] * jnp.exp(old - peak)
        picked = pick_lanes[spot, :]
        for part, hit in zip(parts, hits(spot, c)):
            total = total + jnp.exp(part - peak)
            picked = picked + jnp.where(hit, part, 0.0)
        peak_lanes[spot, :] = peak
        sum_lanes[spot, :] = total
        pick_lanes[spot, :] = picked

    def share(t, send_buf, recv_buf, send_sem, recv_sem, count, mine_at, target):
        recv_buf[t, mine_at] = send_buf[t]

        @pl.loop(1, count)
        def _(k):
            pltpu.make_async_remote_copy(
                src_ref=send_buf.at[t],
                dst_ref=recv_buf.at[t, mine_at],
                send_sem=send_sem.at[t],
                recv_sem=recv_sem.at[t],
                device_id=target(k),
                device_id_type=MESH,
            ).start()

        every = pl.ds(0, count - 1)
        pltpu.make_async_copy(recv_buf.at[t, every], recv_buf.at[t, every], recv_sem.at[t]).wait()
        norms = recv_buf[t, :, :slabs, :]
        top = jnp.max(norms, axis=0)
        norm = top + jnp.log(jnp.sum(jnp.exp(norms - top[None]), axis=0))
        picked = jnp.sum(recv_buf[t, :, slabs:, :], axis=0)
        pltpu.make_async_copy(recv_buf.at[t, every], recv_buf.at[t, every], send_sem.at[t]).wait()
        return norm, picked

    def settle(t):
        for i in range(slabs):
            part = pl.ds(i * LANES, LANES)
            peaks = peak_lanes[part, :].T
            top = jnp.max(peaks, axis=0, keepdims=True)
            total = jnp.sum(sum_lanes[part, :].T * jnp.exp(peaks - top), axis=0, keepdims=True)
            row_send[t, i : i + 1, :] = top + jnp.log(total)
            row_send[t, slabs + i : slabs + i + 1, :] = jnp.sum(
                pick_lanes[part, :].T, axis=0, keepdims=True
            )
        norm, picked = share(
            t, row_send, row_recv, row_out, row_in, row_n, my_row,
            lambda k: (my_cls, lax.rem(my_row + k, row_n)),
        )
        cls_send[t, :slabs, :] = norm
        cls_send[t, slabs:, :] = picked
        norm, picked = share(
            t, cls_send, cls_recv, cls_out, cls_in, cls_n, my_cls,
            lambda k: (lax.rem(my_cls + k, cls_n), my_row),
        )
        loss = norm - picked
        for i in range(slabs):
            losses_ref[t : t + 1, i * LANES : (i + 1) * LANES] = loss[i : i + 1, :]
            norm_lanes[pl.ds(i * LANES, LANES), :] = jnp.broadcast_to(
                norm[i : i + 1, :], (LANES, LANES)
            ).T

    def residual(c, spot, earlier):
        norm = norm_lanes[spot, :]
        block = logits[c, spot, :]
        for q, hit in enumerate(hits(spot, c)):
            columns = slice(q * LANES, (q + 1) * LANES)
            value = jnp.exp(block[:, columns] - norm) - jnp.where(hit, 1.0, 0.0)
            if earlier:
                value = value + total_ref[c, spot, columns].astype(jnp.float32)
            total_ref[c, spot, columns] = value.astype(jnp.bfloat16)

    reset()

    @pl.loop(0, chunks)
    def _(c):
        arrived = pl.ds(0, (n - 1) * features)
        pltpu.make_async_copy(
            incoming.at[c, arrived], incoming.at[c, arrived], in_sem.at[c]
        ).wait()

        @pl.loop(0, tiles)
        def _(i):
            here = pl.ds(pl.multiple_of(i * ROW_TILE, ROW_TILE), ROW_TILE)
            logits[c, here, :] = jnp.dot(
                examples[here, :], incoming[c], preferred_element_type=jnp.float32
            )

            @pl.loop(0, ROW_TILE // SUB, unroll=2)
            def _(u):
                spot = pl.ds(pl.multiple_of(i * ROW_TILE + u * SUB, SUB), SUB)
                collect(c, spot, logits[c, spot, :])

    settle(0)
    reset()

    @pl.loop(0, rows // SUB, unroll=4)
    def _(u):
        residual(0, pl.ds(pl.multiple_of(u * SUB, SUB), SUB), False)

    for c in range(chunks):
        for i in range(tiles):
            here = pl.ds(i * ROW_TILE, ROW_TILE)
            change = jnp.dot(gram[here, :], total_ref[c], preferred_element_type=jnp.float32)
            if c + 1 < chunks:
                residual(c + 1, here, False)
            block = logits[c, here, :] - rate * change
            logits[c, here, :] = block
            collect(c, here, block)

    settle(1)

    @pl.loop(0, chunks)
    def _(c):
        @pl.loop(0, rows // SUB, unroll=4)
        def _(u):
            residual(c, pl.ds(pl.multiple_of(u * SUB, SUB), SUB), True)

    pltpu.make_async_copy(examples.at[peers], examples.at[peers], emb_out).wait()

    @pl.loop(0, chunks)
    def _(c):
        sent = pl.ds(0, n - 1)
        pltpu.make_async_copy(outgoing.at[c, sent], outgoing.at[c, sent], out_sem.at[c]).wait()


def update_kernel(rate, turned_ref, total_ref, out_ref):
    out_ref[...] = -rate * jnp.dot(
        turned_ref[...], total_ref[0], preferred_element_type=jnp.float32
    )


def fused(embeddings, weights, labels):
    cls_n, row_n = lax.axis_size("cls"), lax.axis_size("row")
    n = cls_n * row_n
    shard_rows, model_width = embeddings.shape
    rows = shard_rows * row_n
    features = weights.shape[0]
    class_count = weights.shape[1] // n
    width = max(w for w in (128, 256, 384, 512) if class_count % w == 0)
    chunks = class_count // width
    rate = learn_rate / rows
    slabs = rows // LANES
    vmem = pl.BlockSpec(memory_space=pltpu.VMEM)
    dma = pltpu.SemaphoreType.DMA
    total, turned, losses = pl.pallas_call(
        functools.partial(exchange_kernel, cls_n, row_n, rate),
        out_shape=(
            jax.ShapeDtypeStruct((chunks, rows, width), jnp.bfloat16),
            jax.ShapeDtypeStruct((model_width, rows), jnp.bfloat16),
            jax.ShapeDtypeStruct((STEPS, rows), jnp.float32),
        ),
        in_specs=[vmem, pl.BlockSpec(memory_space=pl.ANY), vmem],
        out_specs=(vmem, vmem, vmem),
        scratch_shapes=[
            pltpu.VMEM((2, n, features, width), jnp.float32),
            pltpu.VMEM((chunks, n, features, width), jnp.bfloat16),
            pltpu.VMEM((chunks, n * features, width), jnp.bfloat16),
            pltpu.VMEM((rows, LANES), jnp.int32),
            pltpu.VMEM((chunks, rows, width), jnp.float32),
            pltpu.VMEM((rows, rows), jnp.bfloat16),
            pltpu.VMEM((rows, model_width), jnp.bfloat16),
            pltpu.VMEM((shard_rows, model_width), jnp.bfloat16),
            pltpu.VMEM((rows, LANES), jnp.float32),
            pltpu.VMEM((rows, LANES), jnp.float32),
            pltpu.VMEM((rows, LANES), jnp.float32),
            pltpu.VMEM((rows, LANES), jnp.float32),
            pltpu.VMEM((STEPS, 2 * slabs, LANES), jnp.float32),
            pltpu.VMEM((STEPS, row_n, 2 * slabs, LANES), jnp.float32),
            pltpu.VMEM((STEPS, 2 * slabs, LANES), jnp.float32),
            pltpu.VMEM((STEPS, cls_n, 2 * slabs, LANES), jnp.float32),
            dma((2,)),
            dma((chunks,)),
            dma((chunks,)),
            dma,
            dma,
            dma((STEPS,)),
            dma((STEPS,)),
            dma((STEPS,)),
            dma((STEPS,)),
        ],
        compiler_params=pltpu.CompilerParams(
            collective_id=0, has_side_effects=True, vmem_limit_bytes=60 * 1024 * 1024
        ),
    )(embeddings, weights, labels.reshape(slabs, LANES))
    tall = model_width // 2
    update = pl.pallas_call(
        functools.partial(update_kernel, rate),
        grid=(chunks, 2),
        out_shape=jax.ShapeDtypeStruct((model_width, class_count), jnp.float32),
        in_specs=[
            pl.BlockSpec((tall, rows), lambda c, i: (i, 0)),
            pl.BlockSpec((1, rows, width), lambda c, i: (c, 0, 0)),
        ],
        out_specs=pl.BlockSpec((tall, width), lambda c, i: (i, c)),
        compiler_params=pltpu.CompilerParams(
            dimension_semantics=("arbitrary", "arbitrary"), vmem_limit_bytes=60 * 1024 * 1024
        ),
    )(turned, total)
    return update, losses


def shards(embeddings, weights, labels):
    if STEPS == 2 and weights.shape[0] % 16 == 0:
        return fused(embeddings, weights, labels)
    peer_count = lax.axis_size(("cls", "row"))
    examples = lax.all_gather(embeddings.astype(jnp.bfloat16), "row", axis=0, tiled=True)
    row_count = examples.shape[0]
    feature_rows = weights.shape[0]
    class_count = weights.shape[1] // peer_count
    offset = lax.axis_index(("cls", "row")) * class_count
    columns = lax.broadcasted_iota(jnp.int32, (1, class_count), 1) + offset
    label_hit = columns == labels[:, None]
    pieces = weights.astype(jnp.bfloat16).reshape(feature_rows, peer_count, class_count)
    block_weights = lax.all_to_all(
        pieces.transpose(1, 0, 2), ("cls", "row"), split_axis=0, concat_axis=0, tiled=True
    )
    flat_weights = block_weights.reshape(peer_count * feature_rows, class_count)
    first_logits = jnp.dot(examples, flat_weights, preferred_element_type=jnp.float32)
    rate = learn_rate / row_count
    gram = lax.dot_general(
        examples, examples, (((1,), (1,)), ((), ())), preferred_element_type=jnp.float32
    ).astype(jnp.bfloat16)
    total = None
    loss_rows = []
    for step_index in range(STEPS):
        logits = first_logits
        if step_index > 0:
            logits = logits - rate * jnp.dot(gram, total, preferred_element_type=jnp.float32)
        local_peak = jnp.max(logits, axis=1)
        local_total = jnp.sum(jnp.exp(logits - local_peak[:, None]), axis=1)
        local_picked = jnp.sum(jnp.where(label_hit, logits, 0.0), axis=1)
        stats = lax.all_gather(
            jnp.stack([local_peak, local_total, local_picked]), ("cls", "row"), axis=0
        )
        row_peak = jnp.max(stats[:, 0], axis=0)
        row_total = jnp.sum(stats[:, 1] * jnp.exp(stats[:, 0] - row_peak[None, :]), axis=0)
        picked = jnp.sum(stats[:, 2], axis=0)
        log_norm = row_peak + jnp.log(row_total)
        loss_rows.append(log_norm - picked)
        onehot = jnp.where(label_hit, 1.0, 0.0)
        residual = jnp.exp(logits - log_norm[:, None]) - onehot
        if total is not None:
            residual = residual + total.astype(jnp.float32)
        total = residual.astype(jnp.bfloat16)
    update = lax.dot_general(
        examples, total, (((0,), (0,)), ((), ())), preferred_element_type=jnp.float32
    )
    return (-rate * update, jnp.stack(loss_rows))


def solution(mesh):
    placed = (P("row", None), P(("cls", "row"), None), P())
    return jax.shard_map(
        shards,
        mesh=mesh,
        in_specs=placed,
        out_specs=(P(None, ("cls", "row")), P()),
        check_vma=False,
    )
```
